256 devices in a mesh: groups: 4 (over x, y), expert: 64 (over z, core).
Axes of the slice: x: 2, y: 2, z: 32, core: 2. Of those that a mesh axis runs over, the one named last changes fastest.
The devices are a block of a 4x8x32 slice.
Arguments:
- tokens: bfloat16 [2, 16384, 2048], P(None, ('groups', 'expert')), parts along dimension 1, may hold values from -6 to 6
- route_ids: int32 [2, 16384, 2], P(None, ('groups', 'expert')), parts along dimension 1, may hold values from 0 to 63, as said below
- route_slots: int32 [2, 16384, 2], P(None, ('groups', 'expert')), parts along dimension 1, may hold values from 0 to 3, as said below
- mod_shift: float32 [8, 2048], P('groups'), parts along dimension 0, may hold values from -4 to 4
- mod_scale: float32 [8, 2048], P('groups'), parts along dimension 0, may hold values from -4 to 4
- mod_gate: float32 [8, 2048], P('groups'), parts along dimension 0, may hold values from 0.1 to 1.9
- guidance: float32 [4], P('groups'), parts along dimension 0, may hold values from 2 to 6
- router_weight: bfloat16 [2048, 64], replicated, may hold values from -0.125 to 0.125
- expert_gate: bfloat16 [64, 2048, 768], P('expert'), may hold values from -0.125 to 0.125
- expert_up: bfloat16 [64, 2048, 768], P('expert'), may hold values from -0.125 to 0.125
- expert_down: bfloat16 [64, 768, 2048], P('expert'), may hold values from -0.21875 to 0.21875
- shared_gate: bfloat16 [2048, 1408], P('expert'), may hold values from -0.125 to 0.125
- shared_up: bfloat16 [2048, 1408], P('expert'), may hold values from -0.125 to 0.125
- shared_down: bfloat16 [1408, 2048], P(None, 'expert'), may hold values from -0.15625 to 0.15625
- head_weight: bfloat16 [2048, 128], replicated, may hold values from -0.125 to 0.125
Outputs:
- hidden_out: bfloat16 [2, 16384, 2048], P(None, ('groups', 'expert')), parts along dimension 1
- guided: float32 [16384, 128], P(('groups', 'expert')), parts along dimension 0
The draws below stay inside these ranges and needn't reach their ends.
There are 4 independent parts, one for each index of `groups`. The reference program is written for one: setup_inputs(seed, part) draws one part's arguments, and reference() takes and returns one part's arrays. A program takes and returns all parts, laid end to end along the dimension named above; an argument that names none is the same for every part. Nothing has to cross between parts.
Inputs may be any that keep to these rules, and one draw needn't show every extreme that they name: `route_ids`: for each half, the 64 tokens of one device name each expert at most 4 times in all; this is met by some expert on every device, and one expert is named 4 times by every device's tokens of both halves. A token's 2 experts differ. `route_slots`: within one half and one device, the choices that name one expert hold the distinct rows 0 to their number minus 1, in the same place as the expert in route_ids.
All inputs are finite; a program needn't handle non-finite values.
Results may differ from the reference program's by a relative error of at most 0.0067.
Values may be sent and summed in bfloat16 or wider, within the bound.
No kernel may reach another device: no remote copies, remote signals or barrier semaphores. Data moves between devices by JAX's collectives and lax.ppermute only.
A program may use at most 128 MiB of HBM per device.

```python
import jax
import jax.numpy as jnp
from jax import lax

D = 2048
FFE = 768
FS = 1408
TOPK = 2
OUTC = 128
HALF_DEV = 64
EXPERTS = 64
CAP = 4
TOKENS_HALF = 4096
N_EXPERT = 64


def block_routes(block_key, hot_global):
    cost_key, hot_key, order_key = jax.random.split(block_key, 3)
    expert_index = jnp.arange(EXPERTS, dtype=jnp.int32)
    costs = jax.random.randint(cost_key, (EXPERTS,), 3, 10, dtype=jnp.int32)
    hot_local = jax.random.randint(hot_key, (), 0, EXPERTS, dtype=jnp.int32)
    costs = jnp.where((expert_index == hot_global) | (expert_index == hot_local), 1, costs)
    slot_index = jnp.arange(CAP, dtype=jnp.int32)
    ranking = (slot_index[None, :] + 1) * costs[:, None] * EXPERTS + expert_index[:, None]
    ranking = ranking.reshape(-1)
    assigned = TOPK * HALF_DEV
    ranks = jnp.argsort(jnp.argsort(ranking))
    taken = ranks < assigned
    pool = jnp.arange(EXPERTS * CAP, dtype=jnp.int32)
    listed = jnp.sort(jnp.where(taken, pool, EXPERTS * CAP))[:assigned]
    experts_listed = (listed // CAP).reshape(TOPK, HALF_DEV).T
    slots_listed = (listed % CAP).reshape(TOPK, HALF_DEV).T
    shuffle = jax.random.permutation(order_key, HALF_DEV)
    return (experts_listed[shuffle].astype(jnp.int32), slots_listed[shuffle].astype(jnp.int32))


def routing_tables(key):
    base_key = jax.random.fold_in(key, 9103)
    hot_global = jax.random.randint(jax.random.fold_in(base_key, 1), (), 0, EXPERTS, dtype=jnp.int32)
    block_keys = jax.random.split(jax.random.fold_in(base_key, 2), 2 * N_EXPERT)
    chosen_ids, chosen_slots = jax.vmap(block_routes, in_axes=(0, None))(block_keys, hot_global)
    chosen_ids = chosen_ids.reshape(2, N_EXPERT * HALF_DEV, TOPK)
    chosen_slots = chosen_slots.reshape(2, N_EXPERT * HALF_DEV, TOPK)
    return (chosen_ids, chosen_slots)


def draw_route_ids(key, part):
    return routing_tables(key)[0]


def draw_route_slots(key, part):
    return routing_tables(key)[1]


def shard_levels(own_key, shape, cuts, smallest, high):
    def one(axis_at, parts):
        steps = jax.random.uniform(jax.random.fold_in(jax.random.fold_in(own_key, 6), axis_at), (parts,), jnp.float32, smallest / len(cuts), high / len(cuts))
        return jnp.repeat(jnp.exp(steps), shape[axis_at] // parts).reshape((-1,) + (1,) * (len(shape) - axis_at - 1))

    factor_of = one(*cuts[0])
    for cut in cuts[1:]:
        factor_of = factor_of * one(*cut)
    return factor_of


def bell_draw(rng, dims, deviation, limit, pieces=(), kind=jnp.bfloat16):
    entries = jax.random.normal(rng, dims, jnp.float32) * deviation
    if len(pieces) > 0:
        entries = shard_levels(rng, dims, pieces, -0.22, 0.18) * entries
    return jnp.clip(entries, min=-limit, max=limit).astype(kind)


def setup_inputs(seed: int = 0, part: int = 0) -> dict:
    key_of = jax.random.split(jax.random.key(seed), 16)
    part_splits = jax.random.split(jax.random.fold_in(key_of[15], part), 16)
    tokens = bell_draw(part_splits[0], (2, TOKENS_HALF, D), 1.0, 6.0, ((1, 64),))
    route_ids = draw_route_ids(jax.random.fold_in(jax.random.fold_in(key_of[15], part), 71), part)
    route_slots = draw_route_slots(jax.random.fold_in(jax.random.fold_in(key_of[15], part), 71), part)
    mod_shift = bell_draw(part_splits[3], (2, D), 0.5, 4.0, (), jnp.float32)
    mod_scale = bell_draw(part_splits[4], (2, D), 0.5, 4.0, (), jnp.float32)
    mod_gate = jnp.clip(1.0 + 0.18 * jax.random.normal(part_splits[5], (2, D), jnp.float32), 0.1, 1.9)
    guidance = jnp.clip(jax.random.uniform(part_splits[6], (1,), jnp.float32, 2.0, 6.0), 2.0, 6.0)
    router_weight = bell_draw(key_of[7], (D, EXPERTS), D ** -0.5, 0.125)
    expert_gate = bell_draw(key_of[8], (EXPERTS, D, FFE), D ** -0.5, 0.125, ((0, 64),))
    expert_up = bell_draw(key_of[9], (EXPERTS, D, FFE), D ** -0.5, 0.125, ((0, 64),))
    expert_down = bell_draw(key_of[10], (EXPERTS, FFE, D), FFE ** -0.5, 0.21875, ((0, 64),))
    shared_gate = bell_draw(key_of[11], (D, FS), D ** -0.5, 0.125, ((0, 64),))
    shared_up = bell_draw(key_of[12], (D, FS), D ** -0.5, 0.125, ((0, 64),))
    shared_down = bell_draw(key_of[13], (FS, D), FS ** -0.5, 0.15625, ((1, 64),))
    head_weight = bell_draw(key_of[14], (D, OUTC), D ** -0.5, 0.125)
    return dict(tokens=tokens, route_ids=route_ids, route_slots=route_slots, mod_shift=mod_shift, mod_scale=mod_scale, mod_gate=mod_gate, guidance=guidance, router_weight=router_weight, expert_gate=expert_gate, expert_up=expert_up, expert_down=expert_down, shared_gate=shared_gate, shared_up=shared_up, shared_down=shared_down, head_weight=head_weight)


epsilon = 1e-06

def layer_norm(values):
    center = values - lax.optimization_barrier(jnp.mean(values, axis=-1, keepdims=True))
    spread = lax.optimization_barrier(jnp.mean(center * center, axis=-1, keepdims=True))
    return center * lax.rsqrt(spread + epsilon)

def swiglu_rows(row_block, w_gate, w_up, w_down):
    gate_part = jnp.dot(row_block, w_gate, preferred_element_type=jnp.float32)
    up_part = jnp.dot(row_block, w_up, preferred_element_type=jnp.float32)
    hidden = (jax.nn.silu(gate_part) * up_part).astype(jnp.bfloat16)
    return jnp.dot(hidden, w_down, preferred_element_type=jnp.float32)

def one_expert(operands):
    row_block, w_gate, w_up, w_down = operands
    return swiglu_rows(row_block, w_gate, w_up, w_down).astype(jnp.bfloat16)

def reference(tokens, route_ids, route_slots, mod_shift, mod_scale, mod_gate, guidance, router_weight, expert_gate, expert_up, expert_down, shared_gate, shared_up, shared_down, head_weight):
    model_width = tokens.shape[-1]
    inputs = tokens.astype(jnp.float32)
    modulated = (layer_norm(inputs) * (1.0 + mod_scale[:, None, :]) + mod_shift[:, None, :]).astype(jnp.bfloat16)
    flat_rows = modulated.reshape(2 * TOKENS_HALF, model_width)
    logits = jnp.dot(flat_rows, router_weight, preferred_element_type=jnp.float32).reshape(2, TOKENS_HALF, EXPERTS)
    picked = jnp.take_along_axis(logits, route_ids, axis=2)
    affinity = jax.nn.sigmoid(picked)
    weights = affinity / lax.optimization_barrier(jnp.sum(affinity, axis=2, keepdims=True))
    device_of = jnp.arange(TOKENS_HALF, dtype=jnp.int32) // HALF_DEV
    halves = jnp.arange(2, dtype=jnp.int32)
    position = ((halves[:, None, None] * N_EXPERT + device_of[None, :, None]) * EXPERTS + route_ids) * CAP + route_slots
    position = position.reshape(-1).astype(jnp.int32)
    total_rows = 2 * N_EXPERT * EXPERTS * CAP
    sources = jnp.broadcast_to(modulated[:, :, None, :], (2, TOKENS_HALF, TOPK, model_width)).reshape(-1, model_width)
    buffer = jnp.zeros((total_rows, model_width), jnp.bfloat16).at[position].set(sources)
    by_expert = buffer.reshape(2 * N_EXPERT, EXPERTS, CAP, model_width).transpose(1, 0, 2, 3)
    by_expert = by_expert.reshape(EXPERTS, 2 * N_EXPERT * CAP, model_width)
    outputs = lax.map(one_expert, (by_expert, expert_gate, expert_up, expert_down))
    returned = outputs.reshape(EXPERTS, 2 * N_EXPERT, CAP, model_width).transpose(1, 0, 2, 3).reshape(total_rows, model_width)
    chosen = returned[position].reshape(2, TOKENS_HALF, TOPK, model_width).astype(jnp.float32)
    routed = lax.optimization_barrier(jnp.sum(weights[..., None] * chosen, axis=2))
    shared = swiglu_rows(flat_rows, shared_gate, shared_up, shared_down).reshape(2, TOKENS_HALF, model_width)
    hidden_out = (inputs + mod_gate[:, None, :] * (routed + shared)).astype(jnp.bfloat16)
    final_norm = layer_norm(hidden_out.astype(jnp.float32)).astype(jnp.bfloat16)
    predicted = jnp.dot(final_norm.reshape(2 * TOKENS_HALF, model_width), head_weight, preferred_element_type=jnp.float32)
    predicted = predicted.reshape(2, TOKENS_HALF, OUTC)
    guided = predicted[1] + guidance[0] * (predicted[0] - predicted[1])
    return (hidden_out, guided)
```

```python
import jax
import jax.numpy as jnp
from jax import lax
from jax.sharding import PartitionSpec as P

epsilon = 1e-06
lanes = 2


def gather_turned(arrays, axis, dims):
    turned = [jnp.moveaxis(a, dim, 0) for a, dim in zip(arrays, dims)]
    both = jnp.concatenate([t.reshape(len(t), -1) for t in turned], axis=1)
    result, at, gathered = (lax.all_gather(both, axis, axis=0, tiled=True), 0, [])
    for t, dim in zip(turned, dims):
        section = result[:, at : at + t[0].size].reshape(-1, *t.shape[1:])
        gathered.append(jnp.moveaxis(section, 0, dim))
        at += t[0].size
    return tuple(gathered)


def layer_norm(values):
    center = values - jnp.mean(values, axis=-1, keepdims=True)
    spread = jnp.mean(center * center, axis=-1, keepdims=True)
    return center * lax.rsqrt(spread + epsilon)


def mm(a, b):
    return jnp.dot(a, b, preferred_element_type=jnp.float32)


def mm_turned(a, b):
    return lax.dot_general(a, b, (((0,), (0,)), ((), ())), preferred_element_type=jnp.float32)


def descending_rank(extent):
    index = jnp.arange(extent.shape[0], dtype=jnp.int32)
    ahead = (extent[None, :] > extent[:, None]) | (
        (extent[None, :] == extent[:, None]) & (index[None, :] < index[:, None])
    )
    return jnp.sum(ahead.astype(jnp.int32), axis=1)


def build(devices):
    ring = devices // lanes
    reach = ring // 2

    def local(
        tokens,
        route_ids,
        route_slots,
        mod_shift,
        mod_scale,
        mod_gate,
        guidance,
        router_weight,
        expert_gate,
        expert_up,
        expert_down,
        shared_gate,
        shared_up,
        shared_down,
        head_weight,
    ):
        width = tokens.shape[-1]
        per_half = tokens.shape[1]
        rows = 2 * per_half
        choices = route_ids.shape[2]
        experts = router_weight.shape[1]
        capacity = 2 * choices * per_half // experts
        slots = 2 * capacity
        assert experts == devices and expert_gate.shape[0] == 1
        limits = [min(rows, slots * (lanes * (reach - hop) + 1)) for hop in range(reach + 1)]
        column = width // 2
        columns = [slice(0, column), slice(column, width)]

        def shift(values, step):
            pairs = [
                (lanes * z + c, lanes * ((z + step) % ring) + c)
                for z in range(ring)
                for c in range(lanes)
            ]
            return lax.ppermute(values, "expert", pairs)

        def swap(values):
            return lax.ppermute(values, "expert", [(i, i ^ 1) for i in range(devices)])

        full_gate, full_up, full_down = gather_turned(
            (shared_gate, shared_up, shared_down), "expert", (0, 0, 1)
        )

        inputs = tokens.astype(jnp.float32)
        modulated = (
            layer_norm(inputs) * (1.0 + mod_scale[:, None, :]) + mod_shift[:, None, :]
        ).astype(jnp.bfloat16)
        flat = modulated.reshape(rows, width)

        me = lax.axis_index("expert")
        chip, core = me // lanes, me % lanes
        ids = route_ids.reshape(rows, choices)
        half = jnp.arange(rows, dtype=jnp.int32)[:, None] // per_half
        place = (ids * 2 + half) * capacity + route_slots.reshape(rows, choices)
        ahead = (ids // lanes - chip) % ring
        upward = ((ahead >= 1) & (ahead < reach)) | ((ahead == reach) & (ids % lanes == 0))
        downward = (ahead > reach) | ((ahead == reach) & (ids % lanes != 0))
        up_rank = descending_rank(jnp.max(jnp.where(upward, ahead, 0), axis=1))
        down_rank = descending_rank(jnp.max(jnp.where(downward, ring - ahead, 0), axis=1))
        order = jnp.arange(rows, dtype=jnp.int32)
        up_matrix = (order[:, None] == up_rank[None, :]).astype(jnp.bfloat16)
        down_matrix = (order[:, None] == down_rank[None, :]).astype(jnp.bfloat16)
        at = jnp.where(
            upward, up_rank[:, None], jnp.where(downward, down_rank[:, None], order[:, None])
        )

        up_rows = mm(up_matrix, flat).astype(jnp.bfloat16)
        down_rows = mm(down_matrix, flat).astype(jnp.bfloat16)

        logits = mm(flat, router_weight)
        expert_index = jnp.arange(experts, dtype=jnp.int32)
        picked = jnp.sum(
            jnp.where(expert_index == ids[:, :, None], logits[:, None, :], 0.0), axis=2
        )
        affinity = jax.nn.sigmoid(picked)
        weights = affinity / jnp.sum(affinity, axis=1, keepdims=True)

        slot_index = jnp.arange(experts * slots, dtype=jnp.int32)
        matches = slot_index[:, None] == place.reshape(1, rows * choices)
        slot_at = jnp.sum(
            jnp.where(matches, (at + 1).astype(jnp.float32).reshape(1, -1), 0.0), axis=1
        )
        slot_weight = jnp.sum(jnp.where(matches, weights.reshape(1, -1), 0.0), axis=1)
        per_chip = lanes * slots
        line = jnp.concatenate(
            [slot_at.reshape(ring, per_chip) - 1.0, slot_weight.reshape(ring, per_chip)], axis=1
        )
        line = jnp.pad(line, ((0, 0), (0, 128 - 2 * per_chip)))
        line = jnp.broadcast_to(line[:, None, :], (ring, lanes, 128)).reshape(devices, 128)
        table = lax.all_to_all(line, "expert", split_axis=0, concat_axis=0, tiled=True)

        back = jnp.arange(ring, dtype=jnp.int32)
        source = lanes * ((chip - back) % ring)
        table = jnp.take(table, jnp.concatenate([source + core, source + 1 - core]), axis=0)
        mine = table[:ring]

        def own_first(values):
            values = values.reshape(ring, lanes, slots)
            return jnp.where(core == 0, values, values[:, ::-1])

        wanted = own_first(mine[:, :per_chip]).reshape(ring, per_chip)
        pick = (wanted[:, :, None] == order.astype(jnp.float32)).astype(jnp.bfloat16)
        core_of = jnp.where(jnp.arange(per_chip, dtype=jnp.int32) < slots, core, 1 - core)
        own_weight = own_first(mine[:, per_chip : 2 * per_chip])[:, 0]
        other_weight = table[ring:, per_chip : 2 * per_chip].reshape(ring, lanes, slots)
        other_weight = jnp.where(core == 0, other_weight[:, 0], other_weight[:, 1])

        far_up = jnp.where(core_of[:, None] == 0, pick[reach], 0)
        far_down = jnp.where(core_of[:, None] != 0, pick[reach], 0)

        def up_pick(hop):
            return (far_up if hop == reach else pick[hop])[:, : limits[hop]]

        def down_pick(hop):
            return (far_down if hop == reach else pick[ring - hop])[:, : limits[hop]]

        taken = {0: mm(pick[0], flat).astype(jnp.bfloat16)}
        ups = [up_rows[:, c] for c in columns]
        downs = [down_rows[:, c] for c in columns]
        for hop in range(1, reach + 1):
            for i in range(len(columns)):
                ups[i] = shift(ups[i][: limits[hop]], 1)
                downs[i] = shift(downs[i][: limits[hop]], -1)
            up_part = [mm(up_pick(hop), v) for v in ups]
            down_part = [mm(down_pick(hop), v) for v in downs]
            if hop < reach:
                taken[hop] = jnp.concatenate(up_part, axis=1).astype(jnp.bfloat16)
                taken[ring - hop] = jnp.concatenate(down_part, axis=1).astype(jnp.bfloat16)
            else:
                both = [u + d for u, d in zip(up_part, down_part)]
                taken[hop] = jnp.concatenate(both, axis=1).astype(jnp.bfloat16)

        near = [o for o in range(ring) if min(o, ring - o) <= reach // 2]
        far = [o for o in range(ring) if min(o, ring - o) > reach // 2]
        answer = {}
        for batch in (near, far):
            stacked = jnp.stack([taken[o] for o in batch])
            own, other = stacked[:, :slots], swap(stacked[:, slots:])
            block = jnp.concatenate([own, other]).reshape(-1, width)
            gate_part = mm(block, expert_gate[0])
            up_part = mm(block, expert_up[0])
            hidden = (jax.nn.silu(gate_part) * up_part).astype(jnp.bfloat16)
            result = mm(hidden, expert_down[0])
            scale = jnp.concatenate(
                [
                    jnp.stack([own_weight[o] for o in batch]),
                    jnp.stack([other_weight[o] for o in batch]),
                ]
            )
            result = (result.reshape(-1, slots, width) * scale[:, :, None]).astype(jnp.bfloat16)
            own, other = result[: len(batch)], swap(result[len(batch) :])
            both = jnp.concatenate([own, other], axis=1)
            for i, o in enumerate(batch):
                answer[o] = both[i]

        up_sum, down_sum = [None, None], [None, None]
        for hop in range(reach, 0, -1):
            for sums, chosen, o, step in (
                (up_sum, up_pick(hop), hop, -1),
                (down_sum, down_pick(hop), ring - hop, 1),
            ):
                for i, c in enumerate(columns):
                    total = mm_turned(chosen, answer[o][:, c])
                    if sums[i] is not None:
                        short = limits[hop] - sums[i].shape[0]
                        total = total + jnp.pad(sums[i], ((0, short), (0, 0))).astype(jnp.float32)
                    sums[i] = shift(total.astype(jnp.bfloat16), step)
        routed = (
            mm_turned(pick[0], answer[0])
            + jnp.concatenate([mm_turned(up_matrix[: limits[1]], v) for v in up_sum], axis=1)
            + jnp.concatenate([mm_turned(down_matrix[: limits[1]], v) for v in down_sum], axis=1)
        ).reshape(2, per_half, width)

        gate_sum = mm(flat, full_gate)
        up_sum = mm(flat, full_up)
        shared_hidden = (jax.nn.silu(gate_sum) * up_sum).astype(jnp.bfloat16)
        shared = mm(shared_hidden, full_down).reshape(2, per_half, width)

        hidden_out = (inputs + mod_gate[:, None, :] * (routed + shared)).astype(jnp.bfloat16)
        final_norm = layer_norm(hidden_out.astype(jnp.float32)).astype(jnp.bfloat16)
        predicted = mm(final_norm.reshape(rows, width), head_weight)
        predicted = predicted.reshape(2, per_half, head_weight.shape[1])
        guided = predicted[1] + guidance[0] * (predicted[0] - predicted[1])
        return (hidden_out, guided)

    return local


def solution(mesh):
    in_specs = (
        P(None, ("groups", "expert"), None),
        P(None, ("groups", "expert"), None),
        P(None, ("groups", "expert"), None),
        P("groups", None),
        P("groups", None),
        P("groups", None),
        P("groups"),
        P(),
        P("expert", None, None),
        P("expert", None, None),
        P("expert", None, None),
        P("expert", None),
        P("expert", None),
        P(None, "expert"),
        P(),
    )
    out_specs = (P(None, ("groups", "expert"), None), P(("groups", "expert"), None))
    local = build(mesh.shape["expert"])
    return jax.shard_map(local, mesh=mesh, in_specs=in_specs, out_specs=out_specs, check_vma=False)
```

```python
import jax
import jax.numpy as jnp
from jax import lax
from jax.experimental import pallas as pl
from jax.experimental.pallas import tpu as pltpu
from jax.sharding import PartitionSpec as P

epsilon = 1e-06
lanes = 2
spare = 8
wide_hops = 9
interpret = False


def layer_norm(values):
    center = values - jnp.mean(values, axis=-1, keepdims=True)
    spread = jnp.mean(center * center, axis=-1, keepdims=True)
    return center * lax.rsqrt(spread + epsilon)


def mm(a, b):
    return jnp.dot(a, b, preferred_element_type=jnp.float32)


def mm_turned(a, b):
    return lax.dot_general(a, b, (((0,), (0,)), ((), ())), preferred_element_type=jnp.float32)


def mm_across(a, b):
    return lax.dot_general(a, b, (((1,), (1,)), ((), ())), preferred_element_type=jnp.float32)


def descending_rank(extent):
    index = jnp.arange(extent.shape[0], dtype=jnp.int32)
    ahead = (extent[None, :] > extent[:, None]) | (
        (extent[None, :] == extent[:, None]) & (index[None, :] < index[:, None])
    )
    return jnp.sum(ahead.astype(jnp.int32), axis=1)


def take_kernel(spot_ref, *refs, slots, experts, count):
    blocks, (rows_ref, scale_ref, pick_ref) = refs[:-3], refs[-3:]
    fields = experts * slots
    head = blocks[0][0:spare, :].astype(jnp.float32)
    if len(blocks) > 1:
        head = jnp.concatenate([head, blocks[1][0:spare, :].astype(jnp.float32)], axis=1)
    line = lax.broadcasted_iota(jnp.int32, (count, fields), 0)
    lane = lax.broadcasted_iota(jnp.int32, (count, fields), 1)
    place = line % slots + jnp.where(line < lanes * slots, spot_ref[0], spot_ref[1]) * slots
    first = (line // slots) % lanes == 0
    hit = lane == place

    def field(k):
        values = head[:, k * fields : (k + 1) * fields]
        values = jnp.where(first, values[0:1, :], values[1:2, :])
        return jnp.sum(jnp.where(hit, values, 0.0), axis=1, keepdims=True)

    at = field(0).astype(jnp.int32)
    length = blocks[0].shape[0]
    stop = lax.broadcasted_iota(jnp.int32, (count, length), 1) - spare
    pick = ((stop == at) & (stop >= 0)).astype(jnp.float32).astype(jnp.bfloat16)
    pick_ref[...] = pick
    scale_ref[...] = jnp.broadcast_to(field(1) + field(2) + field(3), scale_ref.shape)
    start = 0
    for block in blocks:
        part = jnp.dot(pick, block[...], preferred_element_type=jnp.float32)
        rows_ref[:, start : start + block.shape[1]] = part.astype(jnp.bfloat16)
        start += block.shape[1]


def take(spot, blocks, slots, experts, count):
    width = sum(b.shape[1] for b in blocks)
    whole = pl.BlockSpec(memory_space=pltpu.VMEM)
    return pl.pallas_call(
        lambda *refs: take_kernel(*refs, slots=slots, experts=experts, count=count),
        out_shape=(
            jax.ShapeDtypeStruct((count, width), jnp.bfloat16),
            jax.ShapeDtypeStruct((count, 128), jnp.float32),
            jax.ShapeDtypeStruct((count, blocks[0].shape[0]), jnp.bfloat16),
        ),
        in_specs=[pl.BlockSpec(memory_space=pltpu.SMEM)] + [whole] * len(blocks),
        out_specs=(whole, whole, whole),
        name="take_rows",
        interpret=interpret,
    )(spot, *blocks)


def build(devices, groups):
    ring = devices // lanes
    reach = ring // 2

    def local(
        tokens,
        route_ids,
        route_slots,
        mod_shift,
        mod_scale,
        mod_gate,
        guidance,
        router_weight,
        expert_gate,
        expert_up,
        expert_down,
        shared_gate,
        shared_up,
        shared_down,
        head_weight,
    ):
        width = tokens.shape[-1]
        per_half = tokens.shape[1]
        rows = 2 * per_half
        choices = route_ids.shape[2]
        experts = router_weight.shape[1]
        capacity = 2 * choices * per_half // experts
        slots = 2 * capacity
        per_chip = lanes * slots
        fields = experts * slots
        assert experts == devices and expert_gate.shape[0] == 1
        assert 4 * fields == width and shared_gate.shape[0] % groups == 0
        limits = [
            spare + lanes * min(rows, per_chip * (reach - hop) + slots) for hop in range(reach + 1)
        ]
        column = width // 2
        me = lax.axis_index("expert")
        chip, core = me // lanes, me % lanes

        def forth(values, step):
            pairs = [
                (lanes * z + c, lanes * ((z + (step if c == 0 else -step)) % ring) + c)
                for z in range(ring)
                for c in range(lanes)
            ]
            return lax.ppermute(values, "expert", pairs)

        def swap(values):
            return lax.ppermute(values, "expert", [(i, i ^ 1) for i in range(devices)])

        share = shared_gate.shape[0] // groups
        piece = jnp.concatenate([shared_gate, shared_up, shared_down.T], axis=1)
        piece = lax.dynamic_slice_in_dim(piece, lax.axis_index("groups") * share, share, 0)
        same_core = [[lanes * z + c for z in range(ring)] for c in range(lanes)]
        piece = lax.all_gather(piece, "expert", axis=0, tiled=True, axis_index_groups=same_core)
        shared_own = lax.all_gather(piece, "groups", axis=0, tiled=True)
        shared_other = swap(shared_own)

        ids = route_ids.reshape(rows, choices)
        half = jnp.arange(rows, dtype=jnp.int32)[:, None] // per_half
        place = (ids * 2 + half) * capacity + route_slots.reshape(rows, choices)
        packed = jnp.pad(place.T.astype(jnp.float32), ((0, 8 - choices), (0, 0)))
        place_other = swap(packed)[:choices].T.astype(jnp.int32)
        chip_place = jnp.concatenate([place, place_other])
        chip_ids = chip_place // slots

        inputs = tokens.astype(jnp.float32)
        modulated = (
            layer_norm(inputs) * (1.0 + mod_scale[:, None, :]) + mod_shift[:, None, :]
        ).astype(jnp.bfloat16)
        flat = modulated.reshape(rows, width)
        chip_rows = jnp.concatenate([flat, swap(flat)])

        ahead = chip_ids // lanes - chip
        ahead = jnp.where(core == 0, ahead, -ahead) % ring
        goes = ((ahead >= 1) & (ahead < reach)) | ((ahead == reach) & (chip_ids % lanes == core))
        rank = descending_rank(jnp.max(jnp.where(goes, ahead, 0), axis=1))
        order = jnp.arange(lanes * rows, dtype=jnp.int32)
        sort = (order[:, None] == rank[None, :]).astype(jnp.bfloat16)
        sorted_rows = mm(sort, chip_rows).astype(jnp.bfloat16)

        logits = mm(chip_rows, router_weight)
        expert_index = jnp.arange(experts, dtype=jnp.int32)
        picked = jnp.sum(
            jnp.where(expert_index == chip_ids[:, :, None], logits[:, None, :], 0.0), axis=2
        )
        affinity = jax.nn.sigmoid(picked)
        weights = affinity / jnp.sum(affinity, axis=1, keepdims=True)

        slot_index = jnp.arange(fields, dtype=jnp.int32)
        matches = slot_index == chip_place[:, :, None]

        def by_slot(values):
            values = jnp.sum(jnp.where(matches, values, 0.0), axis=1)
            return jnp.sum(values.reshape(lanes, rows, fields), axis=1)

        slot_at = by_slot((rank[:, None, None] + 1).astype(jnp.float32)) - 1.0
        slot_weight = by_slot(weights[:, :, None])
        high = lax.reduce_precision(slot_weight, 8, 7)
        middle = lax.reduce_precision(slot_weight - high, 8, 7)
        low = slot_weight - high - middle
        head = jnp.concatenate([slot_at, high, middle, low], axis=1).astype(jnp.bfloat16)
        stream = jnp.concatenate([jnp.pad(head, ((0, spare - lanes), (0, 0))), sorted_rows])
        spot = jnp.stack([lanes * chip + core, lanes * chip + 1 - core]).astype(jnp.int32)

        taken, scales, picks = {}, {}, {}
        taken[0], scales[0], picks[0] = take(spot, [stream], slots, experts, per_chip)
        blocks = [stream[:, :column], stream[:, column:]]
        for hop in range(1, reach + 1):
            if hop == wide_hops + 1:
                blocks = [jnp.concatenate([b[: limits[hop]] for b in blocks], axis=1)]
            blocks = [forth(b[: limits[hop]], 1) for b in blocks]
            count = lanes * per_chip if hop < reach else per_chip
            taken[hop], scales[hop], picks[hop] = take(spot, blocks, slots, experts, count)

        answer = {}
        for batch in (range(0, reach // 2 + 1), range(reach // 2 + 1, reach + 1)):
            shared_hops = [hop for hop in batch if 0 < hop < reach]
            other = swap(jnp.stack([taken[hop][per_chip:] for hop in shared_hops]))
            block = jnp.concatenate(
                [taken[hop][:per_chip] for hop in batch] + [other.reshape(-1, width)]
            )
            gate_part = mm(block, expert_gate[0])
            up_part = mm(block, expert_up[0])
            hidden = (jax.nn.silu(gate_part) * up_part).astype(jnp.bfloat16)
            result = mm(hidden, expert_down[0]).astype(jnp.bfloat16)
            own = result[: len(batch) * per_chip].reshape(-1, per_chip, width)
            other = swap(result[len(batch) * per_chip :]).reshape(-1, per_chip, width)
            for i, hop in enumerate(batch):
                parts = [own[i]]
                if hop in shared_hops:
                    parts.append(other[shared_hops.index(hop)])
                values = jnp.concatenate(parts).astype(jnp.float32) * scales[hop][:, :1]
                answer[hop] = values.astype(jnp.bfloat16)

        sums = [None]
        for hop in range(reach, 0, -1):
            if hop == wide_hops:
                sums = [sums[0][:, :column], sums[0][:, column:]]
            size = width // len(sums)
            for i in range(len(sums)):
                total = mm_turned(picks[hop], answer[hop][:, i * size : (i + 1) * size])
                if sums[i] is not None:
                    short = limits[hop] - sums[i].shape[0]
                    total = total + jnp.pad(sums[i], ((0, short), (0, 0))).astype(jnp.float32)
                sums[i] = forth(total.astype(jnp.bfloat16), -1)
        routed = []
        for i, part in enumerate(sums):
            size = width // len(sums)
            part = part[spare:]
            here = mm_turned(sort[: part.shape[0]], part)
            kept = mm_turned(picks[0][:, spare:], answer[0][:, i * size : (i + 1) * size])
            here = here + mm_turned(sort, kept.astype(jnp.bfloat16))
            routed.append(here[:rows] + swap(here[rows:].astype(jnp.bfloat16)).astype(jnp.float32))
        routed = jnp.concatenate(routed, axis=1).reshape(2, per_half, width)

        block_rows = width // lanes
        feature = jnp.arange(width, dtype=jnp.int32)
        inner = feature % block_rows
        owner = jnp.where(feature < block_rows, core, 1 - core)
        owner = lanes * (inner // share % ring) + owner
        feature_at = (owner * groups + inner // (share * ring)) * share + inner % share
        turn = (jnp.arange(width, dtype=jnp.int32)[:, None] == feature_at[None, :]).astype(jnp.bfloat16)
        turned = mm(flat, turn).astype(jnp.bfloat16)
        hidden_width = shared_gate.shape[1]

        def shared_in(at):
            part = slice(at * hidden_width, (at + 1) * hidden_width)
            return mm(turned[:, :block_rows], shared_own[:, part]) + mm(
                turned[:, block_rows:], shared_other[:, part]
            )

        shared_hidden = (jax.nn.silu(shared_in(0)) * shared_in(1)).astype(jnp.bfloat16)
        shared = jnp.concatenate(
            [mm_across(shared_hidden, w[:, 2 * hidden_width :]) for w in (shared_own, shared_other)],
            axis=1,
        )
        coarse = lax.reduce_precision(shared, 8, 7)
        fine = lax.reduce_precision(shared - coarse, 8, 7)
        shared = mm_across(jnp.concatenate([coarse, fine]).astype(jnp.bfloat16), turn)
        shared = (shared[:rows] + shared[rows:]).reshape(2, per_half, width)

        hidden_out = (inputs + mod_gate[:, None, :] * (routed + shared)).astype(jnp.bfloat16)
        final_norm = layer_norm(hidden_out.astype(jnp.float32)).astype(jnp.bfloat16)
        predicted = mm(final_norm.reshape(rows, width), head_weight)
        predicted = predicted.reshape(2, per_half, head_weight.shape[1])
        guided = predicted[1] + guidance[0] * (predicted[0] - predicted[1])
        return (hidden_out, guided)

    return local


def solution(mesh):
    in_specs = (
        P(None, ("groups", "expert"), None),
        P(None, ("groups", "expert"), None),
        P(None, ("groups", "expert"), None),
        P("groups", None),
        P("groups", None),
        P("groups", None),
        P("groups"),
        P(),
        P("expert", None, None),
        P("expert", None, None),
        P("expert", None, None),
        P("expert", None),
        P("expert", None),
        P(None, "expert"),
        P(),
    )
    out_specs = (P(None, ("groups", "expert"), None), P(("groups", "expert"), None))
    local = build(mesh.shape["expert"], mesh.shape["groups"])
    return jax.shard_map(local, mesh=mesh, in_specs=in_specs, out_specs=out_specs, check_vma=False)
```

```python
import jax
import jax.numpy as jnp
from jax import lax
from jax.experimental import pallas as pl
from jax.experimental.pallas import tpu as pltpu
from jax.sharding import PartitionSpec as P

epsilon = 1e-06
lanes = 2
spare = 8
wide_hops = 12
interpret = False


def layer_norm(values):
    center = values - jnp.mean(values, axis=-1, keepdims=True)
    spread = jnp.mean(center * center, axis=-1, keepdims=True)
    return center * lax.rsqrt(spread + epsilon)


def mm(a, b):
    return jnp.dot(a, b, preferred_element_type=jnp.float32)


def mm_turned(a, b):
    return lax.dot_general(a, b, (((0,), (0,)), ((), ())), preferred_element_type=jnp.float32)


def mm_across(a, b):
    return lax.dot_general(a, b, (((1,), (1,)), ((), ())), preferred_element_type=jnp.float32)


def descending_rank(extent):
    index = jnp.arange(extent.shape[0], dtype=jnp.int32)
    ahead = (extent[None, :] > extent[:, None]) | (
        (extent[None, :] == extent[:, None]) & (index[None, :] < index[:, None])
    )
    return jnp.sum(ahead.astype(jnp.int32), axis=1)


def take_kernel(spot_ref, *refs, slots, experts, count):
    blocks, (rows_ref, scale_ref, pick_ref) = refs[:-3], refs[-3:]
    fields = experts * slots
    head = blocks[0][0:spare, :].astype(jnp.float32)
    if len(blocks) > 1:
        head = jnp.concatenate([head, blocks[1][0:spare, :].astype(jnp.float32)], axis=1)
    line = lax.broadcasted_iota(jnp.int32, (count, fields), 0)
    lane = lax.broadcasted_iota(jnp.int32, (count, fields), 1)
    place = line % slots + jnp.where(line < lanes * slots, spot_ref[0], spot_ref[1]) * slots
    first = (line // slots) % lanes == 0
    hit = lane == place

    def field(k):
        values = head[:, k * fields : (k + 1) * fields]
        values = jnp.where(first, values[0:1, :], values[1:2, :])
        return jnp.sum(jnp.where(hit, values, 0.0), axis=1, keepdims=True)

    at = field(0).astype(jnp.int32)
    length = blocks[0].shape[0]
    stop = lax.broadcasted_iota(jnp.int32, (count, length), 1) - spare
    pick = ((stop == at) & (stop >= 0)).astype(jnp.float32).astype(jnp.bfloat16)
    stop = lax.broadcasted_iota(jnp.int32, pick_ref.shape, 1)
    pick_ref[...] = (stop == at).astype(jnp.float32).astype(jnp.bfloat16)
    scale_ref[...] = jnp.broadcast_to(field(1) + field(2) + field(3), scale_ref.shape)
    start = 0
    for block in blocks:
        part = jnp.dot(pick, block[...], preferred_element_type=jnp.float32)
        rows_ref[:, start : start + block.shape[1]] = part.astype(jnp.bfloat16)
        start += block.shape[1]


def take(spot, blocks, slots, experts, count):
    width = sum(b.shape[1] for b in blocks)
    whole = pl.BlockSpec(memory_space=pltpu.VMEM)
    return pl.pallas_call(
        lambda *refs: take_kernel(*refs, slots=slots, experts=experts, count=count),
        out_shape=(
            jax.ShapeDtypeStruct((count, width), jnp.bfloat16),
            jax.ShapeDtypeStruct((count, width), jnp.float32),
            jax.ShapeDtypeStruct((count, blocks[0].shape[0] - spare), jnp.bfloat16),
        ),
        in_specs=[pl.BlockSpec(memory_space=pltpu.SMEM)] + [whole] * len(blocks),
        out_specs=(whole, whole, whole),
        name="take_rows",
        interpret=interpret,
    )(spot, *blocks)


def join_kernel(*refs, parts):
    start = 0
    for ref, (low, high) in zip(refs[:-1], parts):
        refs[-1][start : start + high - low, :] = ref[low:high, :]
        start += high - low


def join(arrays, parts):
    whole = pl.BlockSpec(memory_space=pltpu.VMEM)
    total = sum(high - low for low, high in parts)
    return pl.pallas_call(
        lambda *refs: join_kernel(*refs, parts=parts),
        out_shape=jax.ShapeDtypeStruct((total, arrays[0].shape[1]), arrays[0].dtype),
        in_specs=[whole] * len(arrays),
        out_specs=whole,
        name="join_rows",
        interpret=interpret,
    )(*arrays)


def build(devices, groups):
    ring = devices // lanes
    reach = ring // 2

    def local(
        tokens,
        route_ids,
        route_slots,
        mod_shift,
        mod_scale,
        mod_gate,
        guidance,
        router_weight,
        expert_gate,
        expert_up,
        expert_down,
        shared_gate,
        shared_up,
        shared_down,
        head_weight,
    ):
        width = tokens.shape[-1]
        per_half = tokens.shape[1]
        rows = 2 * per_half
        choices = route_ids.shape[2]
        experts = router_weight.shape[1]
        capacity = 2 * choices * per_half // experts
        slots = 2 * capacity
        per_chip = lanes * slots
        fields = experts * slots
        assert experts == devices and expert_gate.shape[0] == 1
        assert 4 * fields == width and shared_gate.shape[0] % groups == 0
        limits = [
            spare + lanes * min(rows, per_chip * (reach - hop) + slots) for hop in range(reach + 1)
        ]
        column = width // 2
        me = lax.axis_index("expert")
        chip, core = me // lanes, me % lanes

        def forth(values, step):
            pairs = [
                (lanes * z + c, lanes * ((z + (step if c == 0 else -step)) % ring) + c)
                for z in range(ring)
                for c in range(lanes)
            ]
            return lax.ppermute(values, "expert", pairs)

        def swap(values):
            return lax.ppermute(values, "expert", [(i, i ^ 1) for i in range(devices)])

        share = shared_gate.shape[0] // groups
        piece = jnp.concatenate([shared_gate, shared_up, shared_down.T], axis=1)
        piece = lax.dynamic_slice_in_dim(piece, lax.axis_index("groups") * share, share, 0)
        same_core = [[lanes * z + c for z in range(ring)] for c in range(lanes)]
        piece = lax.all_gather(piece, "expert", axis=0, tiled=True, axis_index_groups=same_core)
        shared_own = lax.all_gather(piece, "groups", axis=0, tiled=True)
        shared_other = swap(shared_own)

        ids = route_ids.reshape(rows, choices)
        half = jnp.arange(rows, dtype=jnp.int32)[:, None] // per_half
        place = (ids * 2 + half) * capacity + route_slots.reshape(rows, choices)
        packed = jnp.pad(place.T.astype(jnp.float32), ((0, 8 - choices), (0, 0)))
        place_other = swap(packed)[:choices].T.astype(jnp.int32)
        chip_place = jnp.concatenate([place, place_other])
        chip_ids = chip_place // slots

        inputs = tokens.astype(jnp.float32)
        modulated = (
            layer_norm(inputs) * (1.0 + mod_scale[:, None, :]) + mod_shift[:, None, :]
        ).astype(jnp.bfloat16)
        flat = modulated.reshape(rows, width)
        chip_rows = jnp.concatenate([flat, swap(flat)])

        ahead = chip_ids // lanes - chip
        ahead = jnp.where(core == 0, ahead, -ahead) % ring
        goes = ((ahead >= 1) & (ahead < reach)) | ((ahead == reach) & (chip_ids % lanes == core))
        rank = descending_rank(jnp.max(jnp.where(goes, ahead, 0), axis=1))
        order = jnp.arange(lanes * rows, dtype=jnp.int32)
        sort = (order[:, None] == rank[None, :]).astype(jnp.bfloat16)
        sorted_rows = mm(sort, chip_rows).astype(jnp.bfloat16)

        logits = mm(chip_rows, router_weight)
        expert_index = jnp.arange(experts, dtype=jnp.int32)
        picked = jnp.sum(
            jnp.where(expert_index == chip_ids[:, :, None], logits[:, None, :], 0.0), axis=2
        )
        affinity = jax.nn.sigmoid(picked)
        weights = affinity / jnp.sum(affinity, axis=1, keepdims=True)

        slot_index = jnp.arange(fields, dtype=jnp.int32)
        matches = slot_index == chip_place[:, :, None]

        def by_slot(values):
            values = jnp.sum(jnp.where(matches, values, 0.0), axis=1)
            return jnp.sum(values.reshape(lanes, rows, fields), axis=1)

        slot_at = by_slot((rank[:, None, None] + 1).astype(jnp.float32)) - 1.0
        slot_weight = by_slot(weights[:, :, None])
        high = lax.reduce_precision(slot_weight, 8, 7)
        middle = lax.reduce_precision(slot_weight - high, 8, 7)
        low = slot_weight - high - middle
        head = jnp.concatenate([slot_at, high, middle, low], axis=1).astype(jnp.bfloat16)
        stream = jnp.concatenate([jnp.pad(head, ((0, spare - lanes), (0, 0))), sorted_rows])
        spot = jnp.stack([lanes * chip + core, lanes * chip + 1 - core]).astype(jnp.int32)

        taken, scales, picks, answer = {}, {}, {}, {}
        near, far = range(0, reach // 2 + 1), range(reach // 2 + 1, reach + 1)

        def expert_in(batch):
            away = (per_chip, lanes * per_chip)
            passed = [taken[hop] for hop in batch if 0 < hop < reach]
            other = swap(join(passed, [away] * len(passed)))
            block = join(
                [taken[hop] for hop in batch] + [other],
                [(0, per_chip)] * len(batch) + [(0, other.shape[0])],
            )
            gate_part = mm(block, expert_gate[0])
            up_part = mm(block, expert_up[0])
            return (jax.nn.silu(gate_part) * up_part).astype(jnp.bfloat16)

        def expert_out(hidden):
            return mm(hidden, expert_down[0]).astype(jnp.bfloat16)

        def answer_batch(result, batch):
            own = result[: len(batch) * per_chip].reshape(-1, per_chip, width)
            other = swap(result[len(batch) * per_chip :]).reshape(-1, per_chip, width)
            passed = [hop for hop in batch if 0 < hop < reach]
            for i, hop in enumerate(batch):
                parts = [own[i]]
                if hop in passed:
                    parts.append(other[passed.index(hop)])
                values = jnp.concatenate(parts).astype(jnp.float32) * scales[hop]
                answer[hop] = values.astype(jnp.bfloat16)

        taken[0], scales[0], picks[0] = take(spot, [stream], slots, experts, per_chip)
        blocks = [stream[:, :column], stream[:, column:]]
        for hop in range(1, reach + 1):
            if hop == wide_hops + 1:
                blocks = [jnp.concatenate([b[: limits[hop]] for b in blocks], axis=1)]
            blocks = [b[: limits[hop]] for b in blocks]
            if hop == reach // 2 + 4:
                blocks[0], hidden = lax.optimization_barrier((blocks[0], expert_in(near)))
            if hop == reach // 2 + 6:
                blocks[0], result = lax.optimization_barrier((blocks[0], expert_out(hidden)))
                answer_batch(result, near)
            for i in range(len(blocks)):
                blocks[i] = forth(blocks[i], 1)
            count = lanes * per_chip if hop < reach else per_chip
            taken[hop], scales[hop], picks[hop] = take(spot, blocks, slots, experts, count)
        answer_batch(expert_out(expert_in(far)), far)

        block_rows = width // lanes
        feature = jnp.arange(width, dtype=jnp.int32)
        inner = feature % block_rows
        owner = jnp.where(feature < block_rows, core, 1 - core)
        owner = lanes * (inner // share % ring) + owner
        feature_at = (owner * groups + inner // (share * ring)) * share + inner % share
        turn = (jnp.arange(width, dtype=jnp.int32)[:, None] == feature_at[None, :]).astype(jnp.bfloat16)
        turned = mm(flat, turn).astype(jnp.bfloat16)
        hidden_width = shared_gate.shape[1]

        def shared_in(at):
            part = slice(at * hidden_width, (at + 1) * hidden_width)
            return mm(turned[:, :block_rows], shared_own[:, part]) + mm(
                turned[:, block_rows:], shared_other[:, part]
            )

        def shared_out(hidden, weights):
            return mm_across(hidden, weights[:, 2 * hidden_width :])

        def shared_back(parts):
            values = jnp.concatenate(parts, axis=1)
            coarse = lax.reduce_precision(values, 8, 7)
            fine = lax.reduce_precision(values - coarse, 8, 7)
            values = mm_across(jnp.concatenate([coarse, fine]).astype(jnp.bfloat16), turn)
            return (values[:rows] + values[rows:]).reshape(2, per_half, width)

        sums = [None]
        for hop in range(reach, 0, -1):
            ahead = None
            if hop == 7:
                ahead = shared_in(0)
            if hop == 6:
                ahead = (
                    jax.nn.silu(shared_gate_part) * shared_in(1)
                ).astype(jnp.bfloat16)
            if hop == 5:
                ahead = [shared_out(shared_hidden, shared_own)]
            if hop == 4:
                ahead = shared_parts + [shared_out(shared_hidden, shared_other)]
            if hop == 3:
                ahead = shared_back(shared_parts)
            if hop == wide_hops:
                sums = [sums[0][:, :column], sums[0][:, column:]]
            size = width // len(sums)
            for i in range(len(sums)):
                total = mm_turned(picks[hop], answer[hop][:, i * size : (i + 1) * size])
                if sums[i] is not None:
                    short = limits[hop] - spare - sums[i].shape[0]
                    total = total + jnp.pad(sums[i], ((0, short), (0, 0))).astype(jnp.float32)
                total = total.astype(jnp.bfloat16)
                if ahead is not None and i == 0:
                    total, ahead = lax.optimization_barrier((total, ahead))
                sums[i] = forth(total, -1)
            if hop == 7:
                shared_gate_part = ahead
            if hop == 6:
                shared_hidden = ahead
            if hop in (5, 4):
                shared_parts = ahead
            if hop == 3:
                shared = ahead
        routed = []
        for i, part in enumerate(sums):
            size = width // len(sums)
            here = mm_turned(sort[: part.shape[0]], part)
            kept = mm_turned(picks[0], answer[0][:, i * size : (i + 1) * size])
            here = here + mm_turned(sort, kept.astype(jnp.bfloat16))
            routed.append(here[:rows] + swap(here[rows:].astype(jnp.bfloat16)).astype(jnp.float32))
        routed = jnp.concatenate(routed, axis=1).reshape(2, per_half, width)

        hidden_out = (inputs + mod_gate[:, None, :] * (routed + shared)).astype(jnp.bfloat16)
        final_norm = layer_norm(hidden_out.astype(jnp.float32)).astype(jnp.bfloat16)
        predicted = mm(final_norm.reshape(rows, width), head_weight)
        predicted = predicted.reshape(2, per_half, head_weight.shape[1])
        guided = predicted[1] + guidance[0] * (predicted[0] - predicted[1])
        return (hidden_out, guided)

    return local


def solution(mesh):
    in_specs = (
        P(None, ("groups", "expert"), None),
        P(None, ("groups", "expert"), None),
        P(None, ("groups", "expert"), None),
        P("groups", None),
        P("groups", None),
        P("groups", None),
        P("groups"),
        P(),
        P("expert", None, None),
        P("expert", None, None),
        P("expert", None, None),
        P("expert", None),
        P("expert", None),
        P(None, "expert"),
        P(),
    )
    out_specs = (P(None, ("groups", "expert"), None), P(("groups", "expert"), None))
    local = build(mesh.shape["expert"], mesh.shape["groups"])

    return jax.shard_map(local, mesh=mesh, in_specs=in_specs, out_specs=out_specs, check_vma=False)
```
